32 devices in a mesh: groups: 2 (over y), expert: 4 (over z), tensor: 2 (over x), sub: 2 (over core).
Axes of the slice: x: 2, y: 2, z: 4, core: 2. Of those that a mesh axis runs over, the one named last changes fastest.
Arguments:
- tokens: bfloat16 [48, 7168], P(('groups', 'expert', 'tensor'), 'sub'), parts along dimension 0, may hold values from -6 to 6
- expert_ids: int32 [48, 8], P(('groups', 'expert', 'tensor')), parts along dimension 0, may hold values from 0 to 15, all different within a row; in each aligned block of 3 rows (0 to 2, 3 to 5, ...) at most 2 rows name the same one
- gate_weights: float32 [48, 8], P(('groups', 'expert', 'tensor')), parts along dimension 0, may hold values from 0.1 to 0.6
- gate_proj: bfloat16 [16, 1024, 7168], P('expert', 'tensor', 'sub'), may hold values from -0.0625 to 0.0625
- up_proj: bfloat16 [16, 1024, 7168], P('expert', 'tensor', 'sub'), may hold values from -0.0625 to 0.0625
- down_proj: bfloat16 [16, 1024, 7168], P('expert', 'tensor', 'sub'), may hold values from -0.1875 to 0.1875
Outputs:
- blended: bfloat16 [48, 7168], P(('groups', 'expert', 'tensor'), 'sub'), parts along dimension 0
The draws below stay inside these ranges and needn't reach their ends.
There are 2 independent parts, one for each index of `groups`. The reference program is written for one: setup_inputs(seed, part) draws one part's arguments, and reference() takes and returns one part's arrays. A program takes and returns all parts, laid end to end along the dimension named above; an argument that names none is the same for every part. Nothing has to cross between parts.
Inputs may be any that keep to these rules, and one draw needn't show every extreme that they name: `expert_ids`: each row names 8 different experts. Among the rows of one owner (aligned blocks of 3 rows) no expert is named by more than 2 rows, a bound that some block reaches.
All inputs are finite; a program needn't handle non-finite values.
Results may differ from the reference program's by a relative error of at most 0.02.
Values may be sent and summed in bfloat16 or wider, within the bound.
A program may use at most 128 MiB of HBM per device.

```python
import math
import jax
import jax.numpy as jnp
import numpy as np
from jax import lax

D = 7168
TOP = 8
FW = 1024
NE = 16
TOK_DEV = 3
SLOTS = 2
TOKENS = 24
N_TENSOR = 2


def levels(own_key, dims, split, low, largest):
    loudness = 1.0
    for position, shards_of in split:
        steps = jax.random.uniform(jax.random.fold_in(jax.random.fold_in(own_key, 6), position), (shards_of,), jnp.float32, low / len(split), largest / len(split))
        loudness = loudness * jnp.repeat(jnp.exp(steps), dims[position] // shards_of).reshape((-1,) + (1,) * (len(dims) - 1 - position))
    return loudness


def routed_block(rng, own, number, rows, number_of, top, bound, lean):
    ranking = jax.random.permutation(rng, number_of)
    heavy_load, common = portions_of(number_of, rows * top, bound, lean, True), portions_of(number_of, rows * top, bound, lean, False)
    places = jnp.arange(number_of)

    def named(tallies, offset_by):
        used = int((tallies > 0).sum())
        fixed = max(1, used // 4)
        passed = fixed + (places - fixed + offset_by * (used - fixed)) % max(1, number_of - fixed)
        return jnp.zeros((number_of,), jnp.int32).at[ranking[jnp.where(places < fixed, places, passed)]].set(jnp.asarray(tallies, jnp.int32))

    tallies = jnp.where(number % 4 == 0, named(heavy_load, number // 4), named(common, number - number // 4 - 1))
    mixed = jax.random.permutation(jax.random.fold_in(own, 3), number_of)
    donor, receiver = mixed[0:number_of // 2 * 2:2], mixed[1:number_of // 2 * 2:2]
    slack = jnp.minimum(tallies[donor] - 1, bound - tallies[receiver]) // 2
    slack = jnp.where((donor == ranking[0]) | (receiver == ranking[0]) | (tallies[receiver] == 0), 0, jnp.maximum(slack, 0))
    passed = jax.random.randint(jax.random.fold_in(own, 4), (number_of // 2,), 0, 1 << 20) % (slack + 1)
    tallies = tallies.at[donor].add(-passed).at[receiver].add(passed)
    items = jnp.searchsorted(jnp.cumsum(tallies), jnp.arange(rows * top), side="right").astype(jnp.int32)
    listing = items.reshape(top, rows).T
    listing = listing[jax.random.permutation(jax.random.fold_in(own, 1), rows)]
    offset_by = jax.random.randint(jax.random.fold_in(own, 2), (rows, 1), 0, top)
    return jnp.take_along_axis(listing, (jnp.arange(top)[None, :] + offset_by) % top, axis=1)


def portions_of(count, total, reach, skew, full):
    loads = [(1 << 20) // math.isqrt(rank ** skew) + 1 for rank in range(1, count + 1)]
    largest = reach if full else min(reach, max(-(-total // count), total * loads[0] // sum(loads)))
    least = 1 if total - largest >= count - 1 else 0
    holding, spare = [largest] + [least] * (count - 1), total - largest - least * (count - 1)
    while spare > 0:
        free = [i for i in range(1, count) if holding[i] < largest] or [i for i in range(1, count) if holding[i] < reach]
        mass, remaining = sum([loads[i] for i in free]), spare
        for i in free:
            extra = min(reach - holding[i], max(1, remaining * loads[i] // mass), spare)
            holding[i] = holding[i] + extra
            spare = spare - extra
    return np.array(holding)


def gaussian(stream_key, dims, scale, most, shards=(), held_as=jnp.bfloat16):
    drawn = scale * jax.random.normal(stream_key, dims, jnp.float32)
    if shards:
        drawn = drawn * levels(stream_key, dims, shards, -0.22, 0.18)
    return jnp.clip(drawn, -most, most).astype(held_as)


def setup_inputs(seed: int = 0, part: int = 0) -> dict:
    seeds = jax.random.split(jax.random.key(seed), 7)
    part_keys = jax.random.split(jax.random.fold_in(seeds[6], part), 7)
    tokens = gaussian(part_keys[0], (TOKENS, D), 1.0, 6.0, ((0, 8), (1, 2)))
    expert_ids_keys = jax.random.split(jax.random.fold_in(part_keys[1], 1), TOKENS // TOK_DEV)
    expert_ids_turns = jax.random.permutation(jax.random.fold_in(part_keys[1], 3), TOKENS // TOK_DEV)
    expert_ids = jax.vmap(lambda own, number: routed_block(jax.random.fold_in(part_keys[1], 2), own, number, TOK_DEV, NE, TOP, SLOTS, 2))(expert_ids_keys, expert_ids_turns).reshape((TOKENS, TOP))
    gate_weights = jnp.clip(0.1 + 0.5 * jax.random.uniform(part_keys[2], (TOKENS, TOP), jnp.float32) ** levels(part_keys[2], (TOKENS, TOP), ((0, 8),), -0.2, 0.2), 0.1, 0.6)
    gate_proj = gaussian(seeds[3], (NE, FW, D), D ** -0.5, 0.0625, ((0, 4), (1, 2), (2, 2)))
    up_proj = gaussian(seeds[4], (NE, FW, D), D ** -0.5, 0.0625, ((0, 4), (1, 2), (2, 2)))
    down_proj = gaussian(seeds[5], (NE, FW, D), FW ** -0.5, 0.1875, ((0, 4), (1, 2), (2, 2)))
    return {"tokens": tokens, "expert_ids": expert_ids, "gate_weights": gate_weights, "gate_proj": gate_proj, "up_proj": up_proj, "down_proj": down_proj}


def reference(tokens, expert_ids, gate_weights, gate_proj, up_proj, down_proj):
    count = tokens.shape[0]
    block = FW // N_TENSOR
    labels = jnp.arange(NE, dtype=jnp.int32)
    chosen = (expert_ids[:, :, None] == labels[None, None, :]).astype(jnp.float32)
    weight_table = jnp.sum(gate_weights[:, :, None].astype(jnp.float32) * chosen, axis=1)
    inputs_wide = tokens.astype(jnp.float32)

    def one_expert(total, inputs):
        gate_rows, up_rows, down_rows, weight_column = inputs
        gate = lax.dot_general(inputs_wide, gate_rows.astype(jnp.float32), (((1,), (1,)), ((), ())), precision=lax.Precision.HIGHEST)
        upper = lax.dot_general(inputs_wide, up_rows.astype(jnp.float32), (((1,), (1,)), ((), ())), precision=lax.Precision.HIGHEST)
        hidden = (jax.nn.silu(gate) * upper).astype(jnp.bfloat16)
        pieces = jnp.einsum("ntf,tfd->ntd", hidden.reshape(count, N_TENSOR, block).astype(jnp.float32), down_rows.reshape(N_TENSOR, block, D).astype(jnp.float32), precision=lax.Precision.HIGHEST)
        pieces = lax.optimization_barrier(pieces.astype(jnp.bfloat16)).astype(jnp.float32)
        expert_out = jnp.sum(pieces, axis=1)
        return total + weight_column[:, None] * expert_out, None

    start = jnp.zeros((count, D), jnp.float32)
    total, unused = lax.scan(one_expert, start, (gate_proj, up_proj, down_proj, weight_table.T))
    return total.astype(jnp.bfloat16)
```

```python
import functools

import jax
import jax.numpy as jnp
from jax import lax
from jax.experimental import pallas as pl
from jax.experimental.pallas import tpu as pltpu
from jax.sharding import PartitionSpec as P

MESH = pl.DeviceIdType.MESH
LANES = 128
IN_TILES = (8, 8, 12)
TURNED = 2
OUT_TILES = (8, 8, 8, 4)
NT = (((1,), (1,)), ((), ()))


def split(tiles, wanted):
    cuts, at = [], 0
    for want in wanted:
        size = min(want, tiles - at)
        if size > 0:
            cuts.append((at, size))
            at += size
    if at < tiles:
        cuts.append((at, tiles - at))
    return cuts


def pad8(rows):
    return pl.cdiv(rows, 8) * 8


def placed_rows(cuts, owned):
    spots, at = [], 0
    for _, tiles in cuts:
        spots.append((at, pad8(owned * tiles)))
        at += spots[-1][1]
    return spots, at


def kernel(
    sizes,
    tok_ref, ids_ref, gw_ref, gate_ref, up_ref, down_ref, out_ref,
    wg, wu, wd, own_tok, own_ids, own_gw, own_table, message, tok_in, table_in, table, wide, x16,
    own_part, sent_part, got_part, hidden, spread, stage, ret, final,
    turned, w_sem, d_sem, own_sem, in_send, in_recv, table_send, table_recv, part_send, part_recv, ret_send, ret_recv,
):
    expert_count, tensor_count, sub_count = sizes
    peers = expert_count * tensor_count
    local_count, units = gate_ref.shape[0], gate_ref.shape[1]
    owned, features = tok_ref.shape
    tiles = features // LANES
    experts = expert_count * local_count
    out_cuts = split(tiles, OUT_TILES)
    out_spots, _ = placed_rows(out_cuts, owned)
    in_cuts = split(tiles, IN_TILES)
    in_spots, in_rows = placed_rows(in_cuts, owned)
    f32, bf16 = jnp.float32, jnp.bfloat16
    expert_at = lax.axis_index("expert")
    me = expert_at * tensor_count + lax.axis_index("tensor")
    sub = lax.axis_index("sub")

    def peer(k):
        p = lax.rem(me + k, peers)
        return p, {"expert": p // tensor_count, "tensor": lax.rem(p, tensor_count)}

    def core(j):
        return {"sub": lax.rem(sub + j, sub_count)}

    def each_peer(body):
        def step(k, carry):
            body(*peer(k))
            return carry

        lax.fori_loop(1, peers, step, 0, unroll=peers <= 16)

    barrier = pltpu.get_barrier_semaphore()
    each_peer(lambda p, where: pl.semaphore_signal(barrier, inc=1, device_id=where, device_id_type=MESH))
    for j in range(1, sub_count):
        pl.semaphore_signal(barrier, inc=1, device_id=core(j), device_id_type=MESH)

    own = [
        pltpu.make_async_copy(src, dst, own_sem.at[i])
        for i, (src, dst) in enumerate(((tok_ref, own_tok), (ids_ref, own_ids), (gw_ref, own_gw)))
    ]
    for copy in own:
        copy.start()
    loads = [
        [
            [
                pltpu.make_async_copy(
                    src.at[l, :, pl.ds(at * LANES, size * LANES)],
                    dst.at[l, :, pl.ds(at * LANES, size * LANES)],
                    w_sem.at[c, l, i],
                )
                for i, (src, dst) in enumerate(((gate_ref, wg), (up_ref, wu)))
            ]
            for l in range(local_count)
        ]
        for c, (at, size) in enumerate(in_cuts)
    ]
    downs = []
    for c, (at, size) in enumerate(out_cuts):
        columns = pl.ds(at * LANES, size * LANES)
        downs.append(pltpu.make_async_copy(down_ref.at[:, :, columns], wd.at[:, :, columns], d_sem.at[c]))
    for chunk in loads:
        for pair in chunk:
            for load in pair:
                load.start(priority=1)
    for load in downs:
        load.start(priority=1)

    own[0].wait()
    mine = own_tok[...].astype(f32)
    wide[pl.ds(0, in_rows), :] = jnp.zeros((in_rows, LANES), f32)
    for (at, size), (spot, _) in zip(in_cuts, in_spots):
        for t in range(size):
            wide[pl.ds(spot + t, owned, size), :] = mine[:, (at + t) * LANES:(at + t + 1) * LANES]
    message[...] = wide[pl.ds(0, in_rows), :].astype(bf16)
    own[1].wait()
    own[2].wait()
    labels = lax.broadcasted_iota(jnp.int32, (owned, experts), 1)
    weights = jnp.zeros((owned, experts), f32)
    for k in range(own_ids.shape[1]):
        weights = weights + jnp.where(own_ids[:, k:k + 1] == labels, own_gw[:, k:k + 1], 0.0)
    own_table[...] = weights

    pl.semaphore_wait(barrier, peers - 1 + sub_count - 1)

    def send_tokens(c):
        spot, rows = in_spots[c]

        def send(p, where):
            pltpu.make_async_remote_copy(
                src_ref=message.at[pl.ds(spot, rows)], dst_ref=tok_in.at[me, pl.ds(spot, rows)],
                send_sem=in_send.at[c], recv_sem=in_recv.at[c], device_id=where, device_id_type=MESH,
            ).start()

        each_peer(send)

    def send_table(p, where):
        pltpu.make_async_remote_copy(
            src_ref=own_table, dst_ref=table_in.at[me], send_sem=table_send, recv_sem=table_recv,
            device_id=where, device_id_type=MESH,
        ).start()

    for c in range(len(in_cuts)):
        send_tokens(c)
    each_peer(send_table)
    tok_in[me] = message[...]
    table_in[me] = own_table[...]
    spread[...] = jnp.zeros_like(spread)

    for c, (at, size) in enumerate(in_cuts[:TURNED]):
        columns = slice(at * LANES, (at + size) * LANES)
        for l in range(local_count):
            for i, w in enumerate((wg, wu)):
                loads[c][l][i].wait()
                turned[2 * l + i, columns, :] = w[l, :, columns].T

    def exchange(l, j):
        return pltpu.make_async_remote_copy(
            src_ref=sent_part.at[l], dst_ref=got_part.at[l, j - 1],
            send_sem=part_send.at[l, j - 1], recv_sem=part_recv.at[l, j - 1],
            device_id=core(j), device_id_type=MESH,
        )

    def gather(c):
        (at, size), (spot, rows) = in_cuts[c], in_spots[c]
        some = tok_in.at[pl.ds(0, peers - 1), pl.ds(spot, rows)]
        pltpu.make_async_copy(some, some, in_recv.at[c]).wait()
        wide[pl.ds(0, peers * rows), :] = (
            tok_in[:, spot:spot + rows, :].astype(f32).reshape(peers * rows, LANES)
        )
        for t in range(size):
            picked = [wide[pl.ds(r * size + t, peers, rows), :] for r in range(owned)]
            x16[:, (at + t) * LANES:(at + t + 1) * LANES] = jnp.concatenate(picked, axis=0).astype(bf16)

    def first(c, l):
        at, size = in_cuts[c]
        columns = slice(at * LANES, (at + size) * LANES)
        x = x16[:, columns]
        for i, w in enumerate((wg, wu)):
            spot = slice(i * units, (i + 1) * units)
            if c < TURNED:
                part = jnp.dot(x, turned[2 * l + i, columns, :], preferred_element_type=f32)
            else:
                part = lax.dot_general(x, w[l, :, columns], NT, preferred_element_type=f32)
            if c > 0:
                part = own_part[l, :, spot] + part
            own_part[l, :, spot] = part
            if c == len(in_cuts) - 1:
                sent_part[l, :, spot] = part.astype(bf16)
        if c == len(in_cuts) - 1:
            for j in range(1, sub_count):
                exchange(l, j).start()

    def finish(l):
        both = own_part[l]
        for j in range(1, sub_count):
            exchange(l, j).wait()
            both = both + got_part[l, j - 1].astype(f32)
        gate, up = both[:, :units], both[:, units:]
        label = expert_at * local_count + l
        chosen = lax.broadcasted_iota(jnp.int32, table.shape, 1) == label
        weight = jnp.sum(jnp.where(chosen, table[...], 0.0), axis=1, keepdims=True)
        hidden[:, l * units:(l + 1) * units] = (gate / (1.0 + jnp.exp(-gate)) * up * weight).astype(bf16)

    last = len(in_cuts) - 1
    for c in range(last):
        gather(c)
        for l in range(local_count):
            if c >= TURNED:
                for load in loads[c][l]:
                    load.wait()
            first(c, l)
    gather(last)
    some = table_in.at[pl.ds(0, peers - 1)]
    pltpu.make_async_copy(some, some, table_recv).wait()
    for r in range(owned):
        table[r * peers:(r + 1) * peers, :] = table_in[:, r, :]
    for l in range(local_count):
        if last >= TURNED:
            for load in loads[last][l]:
                load.wait()
        first(last, l)
        if l > 0:
            finish(l - 1)
    finish(local_count - 1)

    def give(c):
        spot, rows = out_spots[c]

        def send(p, where):
            pltpu.make_async_remote_copy(
                src_ref=stage.at[p, pl.ds(spot, rows)], dst_ref=ret.at[me, pl.ds(spot, rows)],
                send_sem=ret_send.at[c], recv_sem=ret_recv.at[c], device_id=where, device_id_type=MESH,
            ).start()

        each_peer(send)

    for c, (at, size) in enumerate(out_cuts):
        downs[c].wait()
        w = wd[:, :, at * LANES:(at + size) * LANES].reshape(local_count * units, size * LANES)
        part = jnp.dot(hidden[...], w, preferred_element_type=f32)
        spot, rows = out_spots[c]
        for r in range(owned):
            for t in range(size):
                spread[pl.ds(r * size + t, peers, rows), :] = part[
                    r * peers:(r + 1) * peers, t * LANES:(t + 1) * LANES
                ]
        stage[:, spot:spot + rows, :] = spread[: peers * rows, :].reshape(peers, rows, LANES).astype(bf16)
        give(c)

    for c, (at, size) in enumerate(out_cuts):
        spot, rows = out_spots[c]
        some = ret.at[pl.ds(0, peers - 1), pl.ds(spot, rows)]
        pltpu.make_async_copy(some, some, ret_recv.at[c]).wait()
        ret[me, spot:spot + rows, :] = stage[me, spot:spot + rows, :]
        total = jnp.sum(ret[:, spot:spot + rows, :].astype(f32), axis=0)
        for r in range(owned):
            final[pl.ds(at * 8 + r, size, 8), :] = total[r * size:(r + 1) * size]
        for t in range(at, at + size):
            out_ref[:, t * LANES:(t + 1) * LANES] = final[t * 8:t * 8 + owned, :].astype(bf16)

    for c, (spot, rows) in enumerate(in_spots):
        some = tok_in.at[pl.ds(0, peers - 1), pl.ds(spot, rows)]
        pltpu.make_async_copy(some, some, in_send.at[c]).wait()
    some = table_in.at[pl.ds(0, peers - 1)]
    pltpu.make_async_copy(some, some, table_send).wait()
    for c, (spot, rows) in enumerate(out_spots):
        some = ret.at[pl.ds(0, peers - 1), pl.ds(spot, rows)]
        pltpu.make_async_copy(some, some, ret_send.at[c]).wait()


def solution(mesh):
    expert_count, tensor_count = mesh.shape["expert"], mesh.shape["tensor"]
    sub_count = mesh.shape["sub"]
    peers = expert_count * tensor_count

    def per_device(tokens, expert_ids, gate_weights, gate_proj, up_proj, down_proj):
        owned, features = tokens.shape
        top = expert_ids.shape[1]
        local_count, units = gate_proj.shape[0], gate_proj.shape[1]
        rows = peers * owned
        experts = expert_count * local_count
        others = max(1, sub_count - 1)
        tiles = features // LANES
        in_cuts = split(tiles, IN_TILES)
        in_spots, in_rows = placed_rows(in_cuts, owned)
        turned_tiles = sum(size for _, size in in_cuts[:TURNED])
        out_cuts = split(tiles, OUT_TILES)
        out_spots, out_rows = placed_rows(out_cuts, owned)
        widest = max(size for _, size in out_spots)
        pieces = len(out_cuts)
        bf16, f32 = jnp.bfloat16, jnp.float32
        dma = pltpu.SemaphoreType.DMA
        hbm = pl.BlockSpec(memory_space=pl.ANY)
        return pl.pallas_call(
            functools.partial(kernel, (expert_count, tensor_count, sub_count)),
            out_shape=pltpu.VMEM((owned, features), bf16),
            in_specs=[hbm] * 6,
            out_specs=pl.BlockSpec(memory_space=pltpu.VMEM),
            scratch_shapes=[
                pltpu.VMEM(gate_proj.shape, bf16),
                pltpu.VMEM(up_proj.shape, bf16),
                pltpu.VMEM(down_proj.shape, bf16),
                pltpu.VMEM((owned, features), bf16),
                pltpu.VMEM((owned, top), jnp.int32),
                pltpu.VMEM((owned, top), f32),
                pltpu.VMEM((owned, experts), f32),
                pltpu.VMEM((in_rows, LANES), bf16),
                pltpu.VMEM((peers, in_rows, LANES), bf16),
                pltpu.VMEM((peers, owned, experts), f32),
                pltpu.VMEM((rows, experts), f32),
                pltpu.VMEM((peers * max(size for _, size in in_spots), LANES), f32),
                pltpu.VMEM((rows, features), bf16),
                pltpu.VMEM((local_count, rows, 2 * units), f32),
                pltpu.VMEM((local_count, rows, 2 * units), bf16),
                pltpu.VMEM((local_count, others, rows, 2 * units), bf16),
                pltpu.VMEM((rows, local_count * units), bf16),
                pltpu.VMEM((peers * widest, LANES), f32),
                pltpu.VMEM((peers, out_rows, LANES), bf16),
                pltpu.VMEM((peers, out_rows, LANES), bf16),
                pltpu.VMEM((tiles * 8, LANES), f32),
                pltpu.VMEM((2 * local_count, turned_tiles * LANES, units), bf16),
                dma((len(in_cuts), local_count, 2)),
                dma((pieces,)),
                dma((3,)),
                dma((len(in_cuts),)),
                dma((len(in_cuts),)),
                dma(()),
                dma(()),
                dma((local_count, others)),
                dma((local_count, others)),
                dma((pieces,)),
                dma((pieces,)),
            ],
            compiler_params=pltpu.CompilerParams(
                collective_id=0, has_side_effects=True, vmem_limit_bytes=64000 * 1024
            ),
        )(tokens, expert_ids, gate_weights, gate_proj, up_proj, down_proj)

    placed = (
        P(("groups", "expert", "tensor"), "sub"),
        P(("groups", "expert", "tensor"), None),
        P(("groups", "expert", "tensor"), None),
        P("expert", "tensor", "sub"),
        P("expert", "tensor", "sub"),
        P("expert", "tensor", "sub"),
    )
    return jax.shard_map(
        per_device,
        mesh=mesh,
        in_specs=placed,
        out_specs=P(("groups", "expert", "tensor"), "sub"),
        check_vma=False,
    )
```

```python
import functools

import jax
import jax.numpy as jnp
from jax import lax
from jax.experimental import pallas as pl
from jax.experimental.pallas import tpu as pltpu
from jax.sharding import PartitionSpec as P

MESH = pl.DeviceIdType.MESH
LANES = 128
IN_TILES = (8, 8, 12)
AHEAD = 12
SHARE = 3
OUT_TILES = (16, 12)
NT = (((1,), (1,)), ((), ()))


def split(tiles, wanted):
    cuts, at = [], 0
    for want in wanted:
        size = min(want, tiles - at)
        if size > 0:
            cuts.append((at, size))
            at += size
    if at < tiles:
        cuts.append((at, tiles - at))
    return cuts


def pad8(rows):
    return pl.cdiv(rows, 8) * 8


def placed_rows(cuts, owned):
    spots, at = [], 0
    for _, tiles in cuts:
        spots.append((at, pad8(owned * tiles)))
        at += spots[-1][1]
    return spots, at


def turn_plan(cuts, local_count):
    sizes = [size * LANES for _, size in cuts]
    place, beside = {}, {}

    def of(c):
        return [(c, l, i) for l in range(local_count) for i in range(2)]

    for c in range(min(2, len(cuts))):
        for n, job in enumerate(of(c)):
            place[job] = (c, n * sizes[c])
    first = [job for c in range(min(2, len(cuts))) for job in of(c)]
    ahead = max(2 * local_count, AHEAD * local_count // 4)
    now, later = first[:ahead], first[ahead:]
    for n, job in enumerate(later):
        beside.setdefault((0, n * local_count // len(later)), []).append(job)
    if len(cuts) > 2:
        rest = of(2)
        some = min(SHARE * local_count // 4, 2 * local_count * sizes[0] // sizes[2])
        for n, job in enumerate(rest[:some]):
            beside.setdefault((1, n * local_count // some), []).append(job)
            place[job] = (0, n * sizes[2])
        spot, rest = 0, rest[some:]
        for l in range(local_count):
            rest = [job for job in rest if job[1] > l]
            if rest and spot + sizes[2] <= 2 * local_count * sizes[1]:
                beside[2, l] = rest[:1]
                place[rest[0]] = (1, spot)
                spot, rest = spot + sizes[2], rest[1:]
    return now, beside, place


def kernel(
    sizes,
    tok_ref, ids_ref, gw_ref, gate_ref, up_ref, down_ref, out_ref,
    wg, wu, wd, own_tok, own_ids, own_gw, own_table, message, tok_in, table_in, table, wide, x16,
    own_part, sent_part, got_part, hidden, spread, stage, ret, final,
    turned, early, w_sem, d_sem, own_sem, in_send, in_recv, table_send, table_recv, part_send, part_recv, ret_send, ret_recv,
):
    expert_count, tensor_count, sub_count = sizes
    peers = expert_count * tensor_count
    local_count, units = gate_ref.shape[0], gate_ref.shape[1]
    owned, features = tok_ref.shape
    tiles = features // LANES
    experts = expert_count * local_count
    out_cuts = split(tiles, OUT_TILES)
    out_spots, _ = placed_rows(out_cuts, owned)
    in_cuts = split(tiles, IN_TILES)
    in_spots, in_rows = placed_rows(in_cuts, owned)
    f32, bf16 = jnp.float32, jnp.bfloat16
    expert_at = lax.axis_index("expert")
    me = expert_at * tensor_count + lax.axis_index("tensor")
    sub = lax.axis_index("sub")

    def peer(k):
        p = lax.rem(me + k, peers)
        return p, {"expert": p // tensor_count, "tensor": lax.rem(p, tensor_count)}

    def core(j):
        return {"sub": lax.rem(sub + j, sub_count)}

    def each_peer(body):
        def step(k, carry):
            body(*peer(k))
            return carry

        lax.fori_loop(1, peers, step, 0, unroll=peers <= 16)

    barrier = pltpu.get_barrier_semaphore()
    each_peer(lambda p, where: pl.semaphore_signal(barrier, inc=1, device_id=where, device_id_type=MESH))
    for j in range(1, sub_count):
        pl.semaphore_signal(barrier, inc=1, device_id=core(j), device_id_type=MESH)

    own = [
        pltpu.make_async_copy(src, dst, own_sem.at[i])
        for i, (src, dst) in enumerate(((tok_ref, own_tok), (ids_ref, own_ids), (gw_ref, own_gw)))
    ]
    for copy in own:
        copy.start()
    loads = [
        [
            [
                pltpu.make_async_copy(
                    src.at[l, :, pl.ds(at * LANES, size * LANES)],
                    dst.at[l, :, pl.ds(at * LANES, size * LANES)],
                    w_sem.at[c, l, i],
                )
                for i, (src, dst) in enumerate(((gate_ref, wg), (up_ref, wu)))
            ]
            for l in range(local_count)
        ]
        for c, (at, size) in enumerate(in_cuts)
    ]
    downs = []
    for c, (at, size) in enumerate(out_cuts):
        columns = pl.ds(at * LANES, size * LANES)
        downs.append(pltpu.make_async_copy(down_ref.at[:, :, columns], wd.at[:, :, columns], d_sem.at[c]))
    for chunk in loads:
        for pair in chunk:
            for load in pair:
                load.start(priority=1)
    for load in downs:
        load.start(priority=1)

    own[0].wait()
    mine = own_tok[...].astype(f32)
    wide[pl.ds(0, in_rows), :] = jnp.zeros((in_rows, LANES), f32)
    for (at, size), (spot, _) in zip(in_cuts, in_spots):
        for t in range(size):
            wide[pl.ds(spot + t, owned, size), :] = mine[:, (at + t) * LANES:(at + t + 1) * LANES]
    message[...] = wide[pl.ds(0, in_rows), :].astype(bf16)
    own[1].wait()
    own[2].wait()
    labels = lax.broadcasted_iota(jnp.int32, (owned, experts), 1)
    weights = jnp.zeros((owned, experts), f32)
    for k in range(own_ids.shape[1]):
        weights = weights + jnp.where(own_ids[:, k:k + 1] == labels, own_gw[:, k:k + 1], 0.0)
    own_table[...] = weights

    pl.semaphore_wait(barrier, peers - 1 + sub_count - 1)

    def send_tokens(c):
        spot, rows = in_spots[c]

        def send(p, where):
            pltpu.make_async_remote_copy(
                src_ref=message.at[pl.ds(spot, rows)], dst_ref=tok_in.at[me, pl.ds(spot, rows)],
                send_sem=in_send.at[c], recv_sem=in_recv.at[c], device_id=where, device_id_type=MESH,
            ).start()

        each_peer(send)

    def send_table(p, where):
        pltpu.make_async_remote_copy(
            src_ref=own_table, dst_ref=table_in.at[me], send_sem=table_send, recv_sem=table_recv,
            device_id=where, device_id_type=MESH,
        ).start()

    for c in range(len(in_cuts)):
        send_tokens(c)
    each_peer(send_table)
    tok_in[me] = message[...]
    table_in[me] = own_table[...]
    spread[...] = jnp.zeros_like(spread)

    turn_now, turn_beside, turned_at = turn_plan(in_cuts, local_count)

    def turned_unit(job):
        room, row = turned_at[job]
        return turned.at[room, pl.ds(row, in_cuts[job[0]][1] * LANES)]

    def turn(job):
        c, l, i = job
        at, size = in_cuts[c]
        turned_unit(job)[...] = (wg, wu)[i][l, :, at * LANES:(at + size) * LANES].T

    for job in turn_now:
        loads[job[0]][job[1]][job[2]].wait()
        turn(job)

    def exchange(l, j):
        return pltpu.make_async_remote_copy(
            src_ref=sent_part.at[l], dst_ref=got_part.at[l, j - 1],
            send_sem=part_send.at[l, j - 1], recv_sem=part_recv.at[l, j - 1],
            device_id=core(j), device_id_type=MESH,
        )

    def gather(c):
        (at, size), (spot, rows) = in_cuts[c], in_spots[c]
        some = tok_in.at[pl.ds(0, peers - 1), pl.ds(spot, rows)]
        pltpu.make_async_copy(some, some, in_recv.at[c]).wait()
        wide[pl.ds(0, peers * rows), :] = (
            tok_in[:, spot:spot + rows, :].astype(f32).reshape(peers * rows, LANES)
        )
        for t in range(size):
            picked = [wide[pl.ds(r * size + t, peers, rows), :] for r in range(owned)]
            x16[:, (at + t) * LANES:(at + t + 1) * LANES] = jnp.concatenate(picked, axis=0).astype(bf16)

    def first(c, l, half):
        at, size = in_cuts[c]
        columns = slice(at * LANES, (at + size) * LANES)
        x = x16[:, columns]
        for i, w in ((half, (wg, wu)[half]),):
            spot = slice(i * units, (i + 1) * units)
            if (c, l, i) in turned_at:
                part = jnp.dot(x, turned_unit((c, l, i))[...], preferred_element_type=f32)
            else:
                part = lax.dot_general(x, w[l, :, columns], NT, preferred_element_type=f32)
            if c > 0:
                part = own_part[l, :, spot] + part
            own_part[l, :, spot] = part
            if c == len(in_cuts) - 1:
                sent_part[l, :, spot] = part.astype(bf16)
        if c == len(in_cuts) - 1 and half == 1:
            for j in range(1, sub_count):
                exchange(l, j).start()

    def finish(l):
        both = own_part[l]
        for j in range(1, sub_count):
            exchange(l, j).wait()
            both = both + got_part[l, j - 1].astype(f32)
        gate, up = both[:, :units], both[:, units:]
        label = expert_at * local_count + l
        chosen = lax.broadcasted_iota(jnp.int32, table.shape, 1) == label
        weight = jnp.sum(jnp.where(chosen, table[...], 0.0), axis=1, keepdims=True)
        hidden[:, l * units:(l + 1) * units] = (gate / (1.0 + jnp.exp(-gate)) * up * weight).astype(bf16)

    last = len(in_cuts) - 1

    def ready(c, l):
        for i in range(2):
            if (c, l, i) not in turned_at:
                loads[c][l][i].wait()
        for job in turn_beside.get((c, l), ()):
            loads[job[0]][job[1]][job[2]].wait()

    def work(c, l):
        jobs = turn_beside.get((c, l), ())
        first(c, l, 0)
        for job in jobs:
            turn(job)
        first(c, l, 1)

    for c in range(last):
        gather(c)
        for l in range(local_count):
            ready(c, l)
        for l in range(local_count):
            work(c, l)
    gather(last)
    some = table_in.at[pl.ds(0, peers - 1)]
    pltpu.make_async_copy(some, some, table_recv).wait()
    for r in range(owned):
        table[r * peers:(r + 1) * peers, :] = table_in[:, r, :]
    for l in range(local_count):
        ready(last, l)
        work(last, l)
        if l > 1:
            finish(l - 2)
    if local_count > 1:
        finish(local_count - 2)

    def give(c):
        spot, rows = out_spots[c]

        def send(p, where):
            pltpu.make_async_remote_copy(
                src_ref=stage.at[p, pl.ds(spot, rows)], dst_ref=ret.at[me, pl.ds(spot, rows)],
                send_sem=ret_send.at[c], recv_sem=ret_recv.at[c], device_id=where, device_id_type=MESH,
            ).start()

        each_peer(send)

    for c, (at, size) in enumerate(out_cuts):
        downs[c].wait()
        columns = slice(at * LANES, (at + size) * LANES)
        if c == 0:
            done = (local_count - 1) * units
            if local_count > 1:
                w = wd[: local_count - 1, :, columns].reshape(done, size * LANES)
                early[...] = jnp.dot(hidden[:, :done], w, preferred_element_type=f32)
            finish(local_count - 1)
            part = jnp.dot(hidden[:, done:], wd[local_count - 1, :, columns], preferred_element_type=f32)
            if local_count > 1:
                part = early[...] + part
        else:
            w = wd[:, :, columns].reshape(local_count * units, size * LANES)
            part = jnp.dot(hidden[...], w, preferred_element_type=f32)
        spot, rows = out_spots[c]
        for r in range(owned):
            for t in range(size):
                spread[pl.ds(r * size + t, peers, rows), :] = part[
                    r * peers:(r + 1) * peers, t * LANES:(t + 1) * LANES
                ]
        stage[:, spot:spot + rows, :] = spread[: peers * rows, :].reshape(peers, rows, LANES).astype(bf16)
        give(c)

    for c, (at, size) in enumerate(out_cuts):
        spot, rows = out_spots[c]
        some = ret.at[pl.ds(0, peers - 1), pl.ds(spot, rows)]
        pltpu.make_async_copy(some, some, ret_recv.at[c]).wait()
        ret[me, spot:spot + rows, :] = stage[me, spot:spot + rows, :]
        total = jnp.sum(ret[:, spot:spot + rows, :].astype(f32), axis=0)
        for r in range(owned):
            final[pl.ds(at * 8 + r, size, 8), :] = total[r * size:(r + 1) * size]
        for t in range(at, at + size):
            out_ref[:, t * LANES:(t + 1) * LANES] = final[t * 8:t * 8 + owned, :].astype(bf16)

    for c, (spot, rows) in enumerate(in_spots):
        some = tok_in.at[pl.ds(0, peers - 1), pl.ds(spot, rows)]
        pltpu.make_async_copy(some, some, in_send.at[c]).wait()
    some = table_in.at[pl.ds(0, peers - 1)]
    pltpu.make_async_copy(some, some, table_send).wait()
    for c, (spot, rows) in enumerate(out_spots):
        some = ret.at[pl.ds(0, peers - 1), pl.ds(spot, rows)]
        pltpu.make_async_copy(some, some, ret_send.at[c]).wait()


def solution(mesh):
    expert_count, tensor_count = mesh.shape["expert"], mesh.shape["tensor"]
    sub_count = mesh.shape["sub"]
    peers = expert_count * tensor_count

    def per_device(tokens, expert_ids, gate_weights, gate_proj, up_proj, down_proj):
        owned, features = tokens.shape
        top = expert_ids.shape[1]
        local_count, units = gate_proj.shape[0], gate_proj.shape[1]
        rows = peers * owned
        experts = expert_count * local_count
        others = max(1, sub_count - 1)
        tiles = features // LANES
        in_cuts = split(tiles, IN_TILES)
        in_spots, in_rows = placed_rows(in_cuts, owned)
        turned_tiles = max(size for _, size in in_cuts[:2])
        out_cuts = split(tiles, OUT_TILES)
        out_spots, out_rows = placed_rows(out_cuts, owned)
        widest = max(size for _, size in out_spots)
        pieces = len(out_cuts)
        bf16, f32 = jnp.bfloat16, jnp.float32
        dma = pltpu.SemaphoreType.DMA
        hbm = pl.BlockSpec(memory_space=pl.ANY)
        return pl.pallas_call(
            functools.partial(kernel, (expert_count, tensor_count, sub_count)),
            out_shape=pltpu.VMEM((owned, features), bf16),
            in_specs=[hbm] * 6,
            out_specs=pl.BlockSpec(memory_space=pltpu.VMEM),
            scratch_shapes=[
                pltpu.VMEM(gate_proj.shape, bf16),
                pltpu.VMEM(up_proj.shape, bf16),
                pltpu.VMEM(down_proj.shape, bf16),
                pltpu.VMEM((owned, features), bf16),
                pltpu.VMEM((owned, top), jnp.int32),
                pltpu.VMEM((owned, top), f32),
                pltpu.VMEM((owned, experts), f32),
                pltpu.VMEM((in_rows, LANES), bf16),
                pltpu.VMEM((peers, in_rows, LANES), bf16),
                pltpu.VMEM((peers, owned, experts), f32),
                pltpu.VMEM((rows, experts), f32),
                pltpu.VMEM((peers * max(size for _, size in in_spots), LANES), f32),
                pltpu.VMEM((rows, features), bf16),
                pltpu.VMEM((local_count, rows, 2 * units), f32),
                pltpu.VMEM((local_count, rows, 2 * units), bf16),
                pltpu.VMEM((local_count, others, rows, 2 * units), bf16),
                pltpu.VMEM((rows, local_count * units), bf16),
                pltpu.VMEM((peers * widest, LANES), f32),
                pltpu.VMEM((peers, out_rows, LANES), bf16),
                pltpu.VMEM((peers, out_rows, LANES), bf16),
                pltpu.VMEM((tiles * 8, LANES), f32),
                pltpu.VMEM((2, 2 * local_count * turned_tiles * LANES, units), bf16),
                pltpu.VMEM((rows, out_cuts[0][1] * LANES), f32),
                dma((len(in_cuts), local_count, 2)),
                dma((pieces,)),
                dma((3,)),
                dma((len(in_cuts),)),
                dma((len(in_cuts),)),
                dma(()),
                dma(()),
                dma((local_count, others)),
                dma((local_count, others)),
                dma((pieces,)),
                dma((pieces,)),
            ],
            compiler_params=pltpu.CompilerParams(
                collective_id=0, has_side_effects=True, vmem_limit_bytes=64000 * 1024
            ),
        )(tokens, expert_ids, gate_weights, gate_proj, up_proj, down_proj)

    placed = (
        P(("groups", "expert", "tensor"), "sub"),
        P(("groups", "expert", "tensor"), None),
        P(("groups", "expert", "tensor"), None),
        P("expert", "tensor", "sub"),
        P("expert", "tensor", "sub"),
        P("expert", "tensor", "sub"),
    )
    return jax.shard_map(
        per_device,
        mesh=mesh,
        in_specs=placed,
        out_specs=P(("groups", "expert", "tensor"), "sub"),
        check_vma=False,
    )
```

```python
import functools

import jax
import jax.numpy as jnp
from jax import lax
from jax.experimental import pallas as pl
from jax.experimental.pallas import tpu as pltpu
from jax.sharding import PartitionSpec as P

MESH = pl.DeviceIdType.MESH
LANES = 128
IN_TILES = (8, 8, 12)
AHEAD = 12
SHARE = 2
OUT_TILES = (12, 16)
NT = (((1,), (1,)), ((), ()))


def split(tiles, wanted):
    cuts, at = [], 0
    for want in wanted:
        size = min(want, tiles - at)
        if size > 0:
            cuts.append((at, size))
            at += size
    if at < tiles:
        cuts.append((at, tiles - at))
    return cuts


def pad8(rows):
    return pl.cdiv(rows, 8) * 8


def placed_rows(cuts, owned):
    spots, at = [], 0
    for _, tiles in cuts:
        spots.append((at, pad8(owned * tiles)))
        at += spots[-1][1]
    return spots, at


def turn_plan(cuts, local_count):
    sizes = [size * LANES for _, size in cuts]
    place, beside = {}, {}

    def of(c):
        return [(c, l, i) for l in range(local_count) for i in range(2)]

    for c in range(min(2, len(cuts))):
        for n, job in enumerate(of(c)):
            place[job] = (c, n * sizes[c])
    first = [job for c in range(min(2, len(cuts))) for job in of(c)]
    ahead = max(2 * local_count, AHEAD * local_count // 4)
    now, later = first[:ahead], first[ahead:]
    for n, job in enumerate(later):
        beside.setdefault((0, n * local_count // len(later)), []).append(job)
    if len(cuts) > 2:
        rest = of(2)
        some = min(SHARE * local_count // 4, 2 * local_count * sizes[0] // sizes[2])
        for n, job in enumerate(rest[:some]):
            beside.setdefault((1, n * local_count // some), []).append(job)
            place[job] = (0, n * sizes[2])
        spot, rest = 0, rest[some:]
        for l in range(local_count):
            rest = [job for job in rest if job[1] > l]
            if rest and spot + sizes[2] <= 2 * local_count * sizes[1]:
                beside[2, l] = rest[:1]
                place[rest[0]] = (1, spot)
                spot, rest = spot + sizes[2], rest[1:]
    return now, beside, place


def kernel(
    sizes,
    tok_ref, ids_ref, gw_ref, gate_ref, up_ref, down_ref, out_ref,
    wg, wu, wd, own_tok, own_ids, own_gw, own_table, message, tok_in, table_in, table, wide, x16,
    own_part, sent_part, got_part, hidden, spread, stage, ret, final,
    turned, early, marks, w_sem, d_sem, own_sem, in_send, in_recv, table_send, table_recv, part_send, part_recv, ret_send, ret_recv,
):
    expert_count, tensor_count, sub_count = sizes
    peers = expert_count * tensor_count
    local_count, units = gate_ref.shape[0], gate_ref.shape[1]
    owned, features = tok_ref.shape
    tiles = features // LANES
    experts = expert_count * local_count
    out_cuts = split(tiles, OUT_TILES)
    out_spots, _ = placed_rows(out_cuts, owned)
    in_cuts = split(tiles, IN_TILES)
    in_spots, in_rows = placed_rows(in_cuts, owned)
    f32, bf16 = jnp.float32, jnp.bfloat16
    expert_at = lax.axis_index("expert")
    me = expert_at * tensor_count + lax.axis_index("tensor")
    sub = lax.axis_index("sub")

    def peer(k):
        p = lax.rem(me + k, peers)
        return p, {"expert": p // tensor_count, "tensor": lax.rem(p, tensor_count)}

    def core(j):
        return {"sub": lax.rem(sub + j, sub_count)}

    def each_peer(body):
        def step(k, carry):
            body(*peer(k))
            return carry

        lax.fori_loop(1, peers, step, 0, unroll=peers <= 16)

    barrier = pltpu.get_barrier_semaphore()
    each_peer(lambda p, where: pl.semaphore_signal(barrier, inc=1, device_id=where, device_id_type=MESH))
    for j in range(1, sub_count):
        pl.semaphore_signal(barrier, inc=1, device_id=core(j), device_id_type=MESH)

    own = [
        pltpu.make_async_copy(src, dst, own_sem.at[i])
        for i, (src, dst) in enumerate(((tok_ref, own_tok), (ids_ref, own_ids), (gw_ref, own_gw)))
    ]
    for copy in own:
        copy.start()
    loads = [
        [
            [
                pltpu.make_async_copy(
                    src.at[l, :, pl.ds(at * LANES, size * LANES)],
                    dst.at[l, :, pl.ds(at * LANES, size * LANES)],
                    w_sem.at[c, l, i],
                )
                for i, (src, dst) in enumerate(((gate_ref, wg), (up_ref, wu)))
            ]
            for l in range(local_count)
        ]
        for c, (at, size) in enumerate(in_cuts)
    ]
    downs = []
    for c, (at, size) in enumerate(out_cuts):
        columns = pl.ds(at * LANES, size * LANES)
        downs.append(pltpu.make_async_copy(down_ref.at[:, :, columns], wd.at[:, :, columns], d_sem.at[c]))
    for chunk in loads:
        for pair in chunk:
            for load in pair:
                load.start(priority=1)
    for load in downs:
        load.start(priority=1)

    own[0].wait()
    mine = own_tok[...].astype(f32)
    wide[pl.ds(0, in_rows), :] = jnp.zeros((in_rows, LANES), f32)
    for (at, size), (spot, _) in zip(in_cuts, in_spots):
        for t in range(size):
            wide[pl.ds(spot + t, owned, size), :] = mine[:, (at + t) * LANES:(at + t + 1) * LANES]
    message[...] = wide[pl.ds(0, in_rows), :].astype(bf16)
    own[1].wait()
    own[2].wait()
    labels = lax.broadcasted_iota(jnp.int32, (owned, experts), 1)
    weights = jnp.zeros((owned, experts), f32)
    for k in range(own_ids.shape[1]):
        weights = weights + jnp.where(own_ids[:, k:k + 1] == labels, own_gw[:, k:k + 1], 0.0)
    own_table[...] = weights

    pl.semaphore_wait(barrier, peers - 1 + sub_count - 1)

    def send_tokens(c):
        spot, rows = in_spots[c]

        def send(p, where):
            pltpu.make_async_remote_copy(
                src_ref=message.at[pl.ds(spot, rows)], dst_ref=tok_in.at[me, pl.ds(spot, rows)],
                send_sem=in_send.at[c], recv_sem=in_recv.at[c], device_id=where, device_id_type=MESH,
            ).start()

        each_peer(send)

    def send_table(p, where):
        pltpu.make_async_remote_copy(
            src_ref=own_table, dst_ref=table_in.at[me], send_sem=table_send, recv_sem=table_recv,
            device_id=where, device_id_type=MESH,
        ).start()

    each_peer(send_table)
    for c in range(len(in_cuts)):
        send_tokens(c)
    tok_in[me] = message[...]
    table_in[me] = own_table[...]
    spread[...] = jnp.zeros_like(spread)

    turn_now, turn_beside, turned_at = turn_plan(in_cuts, local_count)

    def turned_unit(job):
        room, row = turned_at[job]
        return turned.at[room, pl.ds(row, in_cuts[job[0]][1] * LANES)]

    def turn(job):
        c, l, i = job
        at, size = in_cuts[c]
        turned_unit(job)[...] = (wg, wu)[i][l, :, at * LANES:(at + size) * LANES].T

    for job in turn_now:
        loads[job[0]][job[1]][job[2]].wait()
        turn(job)

    def exchange(l, j):
        return pltpu.make_async_remote_copy(
            src_ref=sent_part.at[l], dst_ref=got_part.at[l, j - 1],
            send_sem=part_send.at[l, j - 1], recv_sem=part_recv.at[l, j - 1],
            device_id=core(j), device_id_type=MESH,
        )

    def gather(c):
        (at, size), (spot, rows) = in_cuts[c], in_spots[c]
        some = tok_in.at[pl.ds(0, peers - 1), pl.ds(spot, rows)]
        pltpu.make_async_copy(some, some, in_recv.at[c]).wait()
        wide[pl.ds(0, peers * rows), :] = (
            tok_in[:, spot:spot + rows, :].astype(f32).reshape(peers * rows, LANES)
        )
        for t in range(size):
            one, two, three = [wide[pl.ds(r * size + t, peers, rows), :] for r in range(owned)]
            for l in range(local_count):
                picked = [jnp.where(marks[l, 0] != 0.0, one, two), jnp.where(marks[l, 1] != 0.0, three, two)]
                x16[l, :, (at + t) * LANES:(at + t + 1) * LANES] = jnp.concatenate(picked, axis=0).astype(bf16)

    def first(c, l, half):
        at, size = in_cuts[c]
        columns = slice(at * LANES, (at + size) * LANES)
        x = x16[l, :, columns]
        for i, w in ((half, (wg, wu)[half]),):
            spot = slice(i * units, (i + 1) * units)
            if (c, l, i) in turned_at:
                part = jnp.dot(x, turned_unit((c, l, i))[...], preferred_element_type=f32)
            else:
                part = lax.dot_general(x, w[l, :, columns], NT, preferred_element_type=f32)
            if c > 0:
                part = own_part[l, :, spot] + part
            own_part[l, :, spot] = part
            if c == len(in_cuts) - 1:
                sent_part[l, :, spot] = part.astype(bf16)
        if c == len(in_cuts) - 1 and half == 1:
            for j in range(1, sub_count):
                exchange(l, j).start()

    def finish(l):
        both = own_part[l]
        for j in range(1, sub_count):
            exchange(l, j).wait()
            both = both + got_part[l, j - 1].astype(f32)
        gate, up = both[:, :units], both[:, units:]
        gated = gate / (1.0 + jnp.exp(-gate)) * up
        first_in, third_in, weight_a, weight_b = [
            jnp.concatenate([marks[l, i]] * (units // LANES), axis=1) for i in range(4)
        ]
        a, b = gated[:peers] * weight_a, gated[peers:] * weight_b
        back = [
            jnp.where(first_in != 0.0, a, 0.0),
            jnp.where(first_in != 0.0, 0.0, a) + jnp.where(third_in != 0.0, 0.0, b),
            jnp.where(third_in != 0.0, b, 0.0),
        ]
        hidden[:, l * units:(l + 1) * units] = jnp.concatenate(back, axis=0).astype(bf16)

    def mark():
        some = table_in.at[pl.ds(0, peers - 1)]
        pltpu.make_async_copy(some, some, table_recv).wait()
        for r in range(owned):
            table[r * peers:(r + 1) * peers, :] = table_in[:, r, :]
        labels = lax.broadcasted_iota(jnp.int32, (peers, experts), 1)
        for l in range(local_count):
            chosen = labels == expert_at * local_count + l
            one, two, three = [
                jnp.sum(jnp.where(chosen, table[r * peers:(r + 1) * peers, :], 0.0), axis=1, keepdims=True)
                for r in range(owned)
            ]
            weight_a = jnp.where(one != 0.0, one, two)
            weight_b = jnp.where(three != 0.0, three, jnp.where(one != 0.0, two, 0.0))
            for i, column in enumerate((one, three, weight_a, weight_b)):
                marks[l, i] = jnp.broadcast_to(column, (peers, LANES))

    last = len(in_cuts) - 1

    def ready(c, l):
        for i in range(2):
            if (c, l, i) not in turned_at:
                loads[c][l][i].wait()
        for job in turn_beside.get((c, l), ()):
            loads[job[0]][job[1]][job[2]].wait()

    def work(c, l):
        jobs = turn_beside.get((c, l), ())
        first(c, l, 0)
        for job in jobs:
            turn(job)
        first(c, l, 1)

    mark()
    for c in range(last):
        gather(c)
        for l in range(local_count):
            ready(c, l)
        for l in range(local_count):
            work(c, l)
    gather(last)
    for l in range(local_count):
        ready(last, l)
        work(last, l)
        if l > 1:
            finish(l - 2)
    if local_count > 1:
        finish(local_count - 2)

    def give(c):
        spot, rows = out_spots[c]

        def send(p, where):
            pltpu.make_async_remote_copy(
                src_ref=stage.at[p, pl.ds(spot, rows)], dst_ref=ret.at[me, pl.ds(spot, rows)],
                send_sem=ret_send.at[c], recv_sem=ret_recv.at[c], device_id=where, device_id_type=MESH,
            ).start()

        each_peer(send)

    for c, (at, size) in enumerate(out_cuts):
        downs[c].wait()
        columns = slice(at * LANES, (at + size) * LANES)
        if c == 0:
            done = (local_count - 1) * units
            if local_count > 1:
                w = wd[: local_count - 1, :, columns].reshape(done, size * LANES)
                early[...] = jnp.dot(hidden[:, :done], w, preferred_element_type=f32)
            finish(local_count - 1)
            part = jnp.dot(hidden[:, done:], wd[local_count - 1, :, columns], preferred_element_type=f32)
            if local_count > 1:
                part = early[...] + part
        else:
            w = wd[:, :, columns].reshape(local_count * units, size * LANES)
            part = jnp.dot(hidden[...], w, preferred_element_type=f32)
        spot, rows = out_spots[c]
        for r in range(owned):
            for t in range(size):
                spread[pl.ds(r * size + t, peers, rows), :] = part[
                    r * peers:(r + 1) * peers, t * LANES:(t + 1) * LANES
                ]
        stage[:, spot:spot + rows, :] = spread[: peers * rows, :].reshape(peers, rows, LANES).astype(bf16)
        give(c)

    for c, (at, size) in enumerate(out_cuts):
        spot, rows = out_spots[c]
        some = ret.at[pl.ds(0, peers - 1), pl.ds(spot, rows)]
        pltpu.make_async_copy(some, some, ret_recv.at[c]).wait()
        ret[me, spot:spot + rows, :] = stage[me, spot:spot + rows, :]
        total = jnp.sum(ret[:, spot:spot + rows, :].astype(f32), axis=0)
        for r in range(owned):
            final[pl.ds(at * 8 + r, size, 8), :] = total[r * size:(r + 1) * size]
        for t in range(at, at + size):
            out_ref[:, t * LANES:(t + 1) * LANES] = final[t * 8:t * 8 + owned, :].astype(bf16)

    for c, (spot, rows) in enumerate(in_spots):
        some = tok_in.at[pl.ds(0, peers - 1), pl.ds(spot, rows)]
        pltpu.make_async_copy(some, some, in_send.at[c]).wait()
    some = table_in.at[pl.ds(0, peers - 1)]
    pltpu.make_async_copy(some, some, table_send).wait()
    for c, (spot, rows) in enumerate(out_spots):
        some = ret.at[pl.ds(0, peers - 1), pl.ds(spot, rows)]
        pltpu.make_async_copy(some, some, ret_send.at[c]).wait()


def solution(mesh):
    expert_count, tensor_count = mesh.shape["expert"], mesh.shape["tensor"]
    sub_count = mesh.shape["sub"]
    peers = expert_count * tensor_count

    def per_device(tokens, expert_ids, gate_weights, gate_proj, up_proj, down_proj):
        owned, features = tokens.shape
        top = expert_ids.shape[1]
        local_count, units = gate_proj.shape[0], gate_proj.shape[1]
        rows = peers * owned
        experts = expert_count * local_count
        others = max(1, sub_count - 1)
        tiles = features // LANES
        in_cuts = split(tiles, IN_TILES)
        in_spots, in_rows = placed_rows(in_cuts, owned)
        turned_tiles = max(size for _, size in in_cuts[:2])
        out_cuts = split(tiles, OUT_TILES)
        out_spots, out_rows = placed_rows(out_cuts, owned)
        widest = max(size for _, size in out_spots)
        pieces = len(out_cuts)
        bf16, f32 = jnp.bfloat16, jnp.float32
        dma = pltpu.SemaphoreType.DMA
        hbm = pl.BlockSpec(memory_space=pl.ANY)
        return pl.pallas_call(
            functools.partial(kernel, (expert_count, tensor_count, sub_count)),
            out_shape=pltpu.VMEM((owned, features), bf16),
            in_specs=[hbm] * 6,
            out_specs=pl.BlockSpec(memory_space=pltpu.VMEM),
            scratch_shapes=[
                pltpu.VMEM(gate_proj.shape, bf16),
                pltpu.VMEM(up_proj.shape, bf16),
                pltpu.VMEM(down_proj.shape, bf16),
                pltpu.VMEM((owned, features), bf16),
                pltpu.VMEM((owned, top), jnp.int32),
                pltpu.VMEM((owned, top), f32),
                pltpu.VMEM((owned, experts), f32),
                pltpu.VMEM((in_rows, LANES), bf16),
                pltpu.VMEM((peers, in_rows, LANES), bf16),
                pltpu.VMEM((peers, owned, experts), f32),
                pltpu.VMEM((rows, experts), f32),
                pltpu.VMEM((peers * max(size for _, size in in_spots), LANES), f32),
                pltpu.VMEM((local_count, 2 * peers, features), bf16),
                pltpu.VMEM((local_count, 2 * peers, 2 * units), f32),
                pltpu.VMEM((local_count, 2 * peers, 2 * units), bf16),
                pltpu.VMEM((local_count, others, 2 * peers, 2 * units), bf16),
                pltpu.VMEM((rows, local_count * units), bf16),
                pltpu.VMEM((peers * widest, LANES), f32),
                pltpu.VMEM((peers, out_rows, LANES), bf16),
                pltpu.VMEM((peers, out_rows, LANES), bf16),
                pltpu.VMEM((tiles * 8, LANES), f32),
                pltpu.VMEM((2, 2 * local_count * turned_tiles * LANES, units), bf16),
                pltpu.VMEM((rows, out_cuts[0][1] * LANES), f32),
                pltpu.VMEM((local_count, 4, peers, LANES), f32),
                dma((len(in_cuts), local_count, 2)),
                dma((pieces,)),
                dma((3,)),
                dma((len(in_cuts),)),
                dma((len(in_cuts),)),
                dma(()),
                dma(()),
                dma((local_count, others)),
                dma((local_count, others)),
                dma((pieces,)),
                dma((pieces,)),
            ],
            compiler_params=pltpu.CompilerParams(
                collective_id=0, has_side_effects=True, vmem_limit_bytes=64000 * 1024
            ),
        )(tokens, expert_ids, gate_weights, gate_proj, up_proj, down_proj)

    placed = (
        P(("groups", "expert", "tensor"), "sub"),
        P(("groups", "expert", "tensor"), None),
        P(("groups", "expert", "tensor"), None),
        P("expert", "tensor", "sub"),
        P("expert", "tensor", "sub"),
        P("expert", "tensor", "sub"),
    )
    return jax.shard_map(
        per_device,
        mesh=mesh,
        in_specs=placed,
        out_specs=P(("groups", "expert", "tensor"), "sub"),
        check_vma=False,
    )
```

```python
import functools

import jax
import jax.numpy as jnp
from jax import lax
from jax.experimental import pallas as pl
from jax.experimental.pallas import tpu as pltpu
from jax.sharding import PartitionSpec as P

MESH = pl.DeviceIdType.MESH
LANES = 128
IN_TILES = (8, 8, 12)
AHEAD = 12
SHARE = 2
OUT_TILES = (12, 16)
NT = (((1,), (1,)), ((), ()))


def split(tiles, wanted):
    cuts, at = [], 0
    for want in wanted:
        size = min(want, tiles - at)
        if size > 0:
            cuts.append((at, size))
            at += size
    if at < tiles:
        cuts.append((at, tiles - at))
    return cuts


def pad8(rows):
    return pl.cdiv(rows, 8) * 8


def placed_rows(cuts, owned):
    spots, at = [], 0
    for _, tiles in cuts:
        spots.append((at, pad8(owned * tiles)))
        at += spots[-1][1]
    return spots, at


def turn_plan(cuts, local_count):
    sizes = [size * LANES for _, size in cuts]
    place, beside = {}, {}

    def of(c):
        return [(c, l, i) for l in range(local_count) for i in range(2)]

    for c in range(min(2, len(cuts))):
        for n, job in enumerate(of(c)):
            place[job] = (c, n * sizes[c])
    first = [job for c in range(min(2, len(cuts))) for job in of(c)]
    ahead = max(2 * local_count, AHEAD * local_count // 4)
    now, later = first[:ahead], first[ahead:]
    for n, job in enumerate(later):
        beside.setdefault((0, n * local_count // len(later)), []).append(job)
    if len(cuts) > 2:
        rest = of(2)
        some = min(SHARE * local_count // 4, 2 * local_count * sizes[0] // sizes[2])
        for n, job in enumerate(rest[:some]):
            beside.setdefault((1, n * local_count // some), []).append(job)
            place[job] = (0, n * sizes[2])
        spot, rest = 0, rest[some:]
        for l in range(local_count):
            rest = [job for job in rest if job[1] > l]
            if rest and spot + sizes[2] <= 2 * local_count * sizes[1]:
                beside[2, l] = rest[:1]
                place[rest[0]] = (1, spot)
                spot, rest = spot + sizes[2], rest[1:]
    return now, beside, place


def kernel(
    sizes,
    tok_ref, ids_ref, gw_ref, gate_ref, up_ref, down_ref, out_ref,
    wg, wu, wd, own_tok, own_ids, own_gw, own_table, message, tok_in, table_in, table, wide, x16,
    own_part, sent_part, got_part, hidden, spread, stage, ret, final,
    turned, early, marks, w_sem, d_sem, own_sem, in_send, in_recv, table_send, table_recv, part_send, part_recv, ret_send, ret_recv,
):
    expert_count, tensor_count, sub_count = sizes
    peers = expert_count * tensor_count
    local_count, units = gate_ref.shape[0], gate_ref.shape[1]
    owned, features = tok_ref.shape
    tiles = features // LANES
    experts = expert_count * local_count
    out_cuts = split(tiles, OUT_TILES)
    out_spots, _ = placed_rows(out_cuts, owned)
    in_cuts = split(tiles, IN_TILES)
    in_spots, in_rows = placed_rows(in_cuts, owned)
    f32, bf16 = jnp.float32, jnp.bfloat16
    expert_at = lax.axis_index("expert")
    me = expert_at * tensor_count + lax.axis_index("tensor")
    sub = lax.axis_index("sub")

    def peer(k):
        p = lax.rem(me + k, peers)
        return p, {"expert": p // tensor_count, "tensor": lax.rem(p, tensor_count)}

    def core(j):
        return {"sub": lax.rem(sub + j, sub_count)}

    def each_peer(body):
        def step(k, carry):
            body(*peer(k))
            return carry

        lax.fori_loop(1, peers, step, 0, unroll=peers <= 16)

    barrier = pltpu.get_barrier_semaphore()
    each_peer(lambda p, where: pl.semaphore_signal(barrier, inc=1, device_id=where, device_id_type=MESH))
    for j in range(1, sub_count):
        pl.semaphore_signal(barrier, inc=1, device_id=core(j), device_id_type=MESH)

    own = [
        pltpu.make_async_copy(src, dst, own_sem.at[i])
        for i, (src, dst) in enumerate(((tok_ref, own_tok), (ids_ref, own_ids), (gw_ref, own_gw)))
    ]
    for copy in own:
        copy.start()
    loads = [
        [
            [
                pltpu.make_async_copy(
                    src.at[l, :, pl.ds(at * LANES, size * LANES)],
                    dst.at[l, :, pl.ds(at * LANES, size * LANES)],
                    w_sem.at[c, l, i],
                )
                for i, (src, dst) in enumerate(((gate_ref, wg), (up_ref, wu)))
            ]
            for l in range(local_count)
        ]
        for c, (at, size) in enumerate(in_cuts)
    ]
    downs = []
    for c, (at, size) in enumerate(out_cuts):
        columns = pl.ds(at * LANES, size * LANES)
        downs.append(pltpu.make_async_copy(down_ref.at[:, :, columns], wd.at[:, :, columns], d_sem.at[c]))
    for chunk in loads:
        for pair in chunk:
            for load in pair:
                load.start(priority=1)
    for load in downs:
        load.start(priority=1)

    own[0].wait()
    mine = own_tok[...].astype(f32)
    wide[pl.ds(0, in_rows), :] = jnp.zeros((in_rows, LANES), f32)
    for (at, size), (spot, _) in zip(in_cuts, in_spots):
        for t in range(size):
            wide[pl.ds(spot + t, owned, size), :] = mine[:, (at + t) * LANES:(at + t + 1) * LANES]
    message[...] = wide[pl.ds(0, in_rows), :].astype(bf16)
    own[1].wait()
    own[2].wait()
    labels = lax.broadcasted_iota(jnp.int32, (owned, experts), 1)
    weights = jnp.zeros((owned, experts), f32)
    for k in range(own_ids.shape[1]):
        weights = weights + jnp.where(own_ids[:, k:k + 1] == labels, own_gw[:, k:k + 1], 0.0)
    own_table[...] = weights

    pl.semaphore_wait(barrier, peers - 1 + sub_count - 1)

    def send_tokens(c):
        spot, rows = in_spots[c]

        def send(p, where):
            pltpu.make_async_remote_copy(
                src_ref=message.at[pl.ds(spot, rows)], dst_ref=tok_in.at[me, pl.ds(spot, rows)],
                send_sem=in_send.at[c], recv_sem=in_recv.at[c], device_id=where, device_id_type=MESH,
            ).start()

        each_peer(send)

    def send_table(p, where):
        pltpu.make_async_remote_copy(
            src_ref=own_table, dst_ref=table_in.at[me], send_sem=table_send, recv_sem=table_recv,
            device_id=where, device_id_type=MESH,
        ).start()

    each_peer(send_table)
    for c in range(len(in_cuts)):
        send_tokens(c)
    tok_in[me] = message[...]
    table_in[me] = own_table[...]
    spread[...] = jnp.zeros_like(spread)

    turn_now, turn_beside, turned_at = turn_plan(in_cuts, local_count)

    def turned_unit(job):
        room, row = turned_at[job]
        return turned.at[room, pl.ds(row, in_cuts[job[0]][1] * LANES)]

    def turn(job):
        c, l, i = job
        at, size = in_cuts[c]
        turned_unit(job)[...] = (wg, wu)[i][l, :, at * LANES:(at + size) * LANES].T

    for job in turn_now:
        loads[job[0]][job[1]][job[2]].wait()
        turn(job)

    def exchange(l, j):
        return pltpu.make_async_remote_copy(
            src_ref=sent_part.at[l], dst_ref=got_part.at[l, j - 1],
            send_sem=part_send.at[l, j - 1], recv_sem=part_recv.at[l, j - 1],
            device_id=core(j), device_id_type=MESH,
        )

    def gather(c):
        (at, size), (spot, rows) = in_cuts[c], in_spots[c]
        some = tok_in.at[pl.ds(0, peers - 1), pl.ds(spot, rows)]
        pltpu.make_async_copy(some, some, in_recv.at[c]).wait()
        wide[pl.ds(0, peers * rows), :] = (
            tok_in[:, spot:spot + rows, :].astype(f32).reshape(peers * rows, LANES)
        )
        for t in range(size):
            one, two, three = [wide[pl.ds(r * size + t, peers, rows), :] for r in range(owned)]
            for l in range(local_count):
                picked = [jnp.where(marks[l, 0] != 0.0, one, two), jnp.where(marks[l, 1] != 0.0, three, two)]
                x16[l, :, (at + t) * LANES:(at + t + 1) * LANES] = jnp.concatenate(picked, axis=0).astype(bf16)

    def first(c, l, half):
        at, size = in_cuts[c]
        columns = slice(at * LANES, (at + size) * LANES)
        x = x16[l, :, columns]
        for i, w in ((half, (wg, wu)[half]),):
            spot = slice(i * units, (i + 1) * units)
            if (c, l, i) in turned_at:
                part = jnp.dot(x, turned_unit((c, l, i))[...], preferred_element_type=f32)
            else:
                part = lax.dot_general(x, w[l, :, columns], NT, preferred_element_type=f32)
            if c > 0:
                part = own_part[l, :, spot] + part
            own_part[l, :, spot] = part
            if c == len(in_cuts) - 1:
                sent_part[l, :, spot] = part.astype(bf16)
        if c == len(in_cuts) - 1 and half == 1:
            for j in range(1, sub_count):
                exchange(l, j).start()

    def finish(l):
        both = own_part[l]
        for j in range(1, sub_count):
            exchange(l, j).wait()
            both = both + got_part[l, j - 1].astype(f32)
        gate, up = both[:, :units], both[:, units:]
        gated = gate / (1.0 + jnp.exp(-gate)) * up
        weight = jnp.concatenate([jnp.concatenate([marks[l, i]] * (units // LANES), axis=1) for i in (2, 3)], axis=0)
        hidden[l] = (gated * weight).astype(bf16)

    def mark():
        some = table_in.at[pl.ds(0, peers - 1)]
        pltpu.make_async_copy(some, some, table_recv).wait()
        for r in range(owned):
            table[r * peers:(r + 1) * peers, :] = table_in[:, r, :]
        labels = lax.broadcasted_iota(jnp.int32, (peers, experts), 1)
        for l in range(local_count):
            chosen = labels == expert_at * local_count + l
            one, two, three = [
                jnp.sum(jnp.where(chosen, table[r * peers:(r + 1) * peers, :], 0.0), axis=1, keepdims=True)
                for r in range(owned)
            ]
            weight_a = jnp.where(one != 0.0, one, two)
            weight_b = jnp.where(three != 0.0, three, jnp.where(one != 0.0, two, 0.0))
            for i, column in enumerate((one, three, weight_a, weight_b)):
                marks[l, i] = jnp.broadcast_to(column, (peers, LANES))

    last = len(in_cuts) - 1

    def ready(c, l):
        for i in range(2):
            if (c, l, i) not in turned_at:
                loads[c][l][i].wait()
        for job in turn_beside.get((c, l), ()):
            loads[job[0]][job[1]][job[2]].wait()

    def work(c, l):
        jobs = turn_beside.get((c, l), ())
        first(c, l, 0)
        for job in jobs:
            turn(job)
        first(c, l, 1)

    mark()
    for c in range(last):
        gather(c)
        for l in range(local_count):
            ready(c, l)
        for l in range(local_count):
            work(c, l)
    gather(last)
    for l in range(local_count):
        ready(last, l)
        work(last, l)
        if l > 1:
            finish(l - 2)
    if local_count > 1:
        finish(local_count - 2)

    def give(c):
        spot, rows = out_spots[c]

        def send(p, where):
            pltpu.make_async_remote_copy(
                src_ref=stage.at[p, pl.ds(spot, rows)], dst_ref=ret.at[me, pl.ds(spot, rows)],
                send_sem=ret_send.at[c], recv_sem=ret_recv.at[c], device_id=where, device_id_type=MESH,
            ).start()

        each_peer(send)

    for c, (at, size) in enumerate(out_cuts):
        downs[c].wait()
        columns = slice(at * LANES, (at + size) * LANES)
        sums = None
        for l in range(local_count):
            if c == 0 and l == local_count - 1:
                if l > 0:
                    early[...] = jnp.concatenate(sums, axis=0)
                finish(l)
                if l > 0:
                    sums = [early[r * peers:(r + 1) * peers, :] for r in range(owned)]
            part = jnp.dot(hidden[l], wd[l, :, columns], preferred_element_type=f32)
            a, b = part[:peers], part[peers:]
            is_one, is_three = [jnp.concatenate([marks[l, i]] * size, axis=1) != 0.0 for i in range(2)]
            back = [
                jnp.where(is_one, a, 0.0),
                jnp.where(is_one, 0.0, a) + jnp.where(is_three, 0.0, b),
                jnp.where(is_three, b, 0.0),
            ]
            sums = back if sums is None else [have + more for have, more in zip(sums, back)]
        spot, rows = out_spots[c]
        for r in range(owned):
            for t in range(size):
                spread[pl.ds(r * size + t, peers, rows), :] = sums[r][:, t * LANES:(t + 1) * LANES]
        stage[:, spot:spot + rows, :] = spread[: peers * rows, :].reshape(peers, rows, LANES).astype(bf16)
        give(c)

    for c, (at, size) in enumerate(out_cuts):
        spot, rows = out_spots[c]
        some = ret.at[pl.ds(0, peers - 1), pl.ds(spot, rows)]
        pltpu.make_async_copy(some, some, ret_recv.at[c]).wait()
        ret[me, spot:spot + rows, :] = stage[me, spot:spot + rows, :]
        total = jnp.sum(ret[:, spot:spot + rows, :].astype(f32), axis=0)
        for r in range(owned):
            final[pl.ds(at * 8 + r, size, 8), :] = total[r * size:(r + 1) * size]
        for t in range(at, at + size):
            out_ref[:, t * LANES:(t + 1) * LANES] = final[t * 8:t * 8 + owned, :].astype(bf16)

    for c, (spot, rows) in enumerate(in_spots):
        some = tok_in.at[pl.ds(0, peers - 1), pl.ds(spot, rows)]
        pltpu.make_async_copy(some, some, in_send.at[c]).wait()
    some = table_in.at[pl.ds(0, peers - 1)]
    pltpu.make_async_copy(some, some, table_send).wait()
    for c, (spot, rows) in enumerate(out_spots):
        some = ret.at[pl.ds(0, peers - 1), pl.ds(spot, rows)]
        pltpu.make_async_copy(some, some, ret_send.at[c]).wait()


def solution(mesh):
    expert_count, tensor_count = mesh.shape["expert"], mesh.shape["tensor"]
    sub_count = mesh.shape["sub"]
    peers = expert_count * tensor_count

    def per_device(tokens, expert_ids, gate_weights, gate_proj, up_proj, down_proj):
        owned, features = tokens.shape
        top = expert_ids.shape[1]
        local_count, units = gate_proj.shape[0], gate_proj.shape[1]
        rows = peers * owned
        experts = expert_count * local_count
        others = max(1, sub_count - 1)
        tiles = features // LANES
        in_cuts = split(tiles, IN_TILES)
        in_spots, in_rows = placed_rows(in_cuts, owned)
        turned_tiles = max(size for _, size in in_cuts[:2])
        out_cuts = split(tiles, OUT_TILES)
        out_spots, out_rows = placed_rows(out_cuts, owned)
        widest = max(size for _, size in out_spots)
        pieces = len(out_cuts)
        bf16, f32 = jnp.bfloat16, jnp.float32
        dma = pltpu.SemaphoreType.DMA
        hbm = pl.BlockSpec(memory_space=pl.ANY)
        return pl.pallas_call(
            functools.partial(kernel, (expert_count, tensor_count, sub_count)),
            out_shape=pltpu.VMEM((owned, features), bf16),
            in_specs=[hbm] * 6,
            out_specs=pl.BlockSpec(memory_space=pltpu.VMEM),
            scratch_shapes=[
                pltpu.VMEM(gate_proj.shape, bf16),
                pltpu.VMEM(up_proj.shape, bf16),
                pltpu.VMEM(down_proj.shape, bf16),
                pltpu.VMEM((owned, features), bf16),
                pltpu.VMEM((owned, top), jnp.int32),
                pltpu.VMEM((owned, top), f32),
                pltpu.VMEM((owned, experts), f32),
                pltpu.VMEM((in_rows, LANES), bf16),
                pltpu.VMEM((peers, in_rows, LANES), bf16),
                pltpu.VMEM((peers, owned, experts), f32),
                pltpu.VMEM((rows, experts), f32),
                pltpu.VMEM((peers * max(size for _, size in in_spots), LANES), f32),
                pltpu.VMEM((local_count, 2 * peers, features), bf16),
                pltpu.VMEM((local_count, 2 * peers, 2 * units), f32),
                pltpu.VMEM((local_count, 2 * peers, 2 * units), bf16),
                pltpu.VMEM((local_count, others, 2 * peers, 2 * units), bf16),
                pltpu.VMEM((local_count, 2 * peers, units), bf16),
                pltpu.VMEM((peers * widest, LANES), f32),
                pltpu.VMEM((peers, out_rows, LANES), bf16),
                pltpu.VMEM((peers, out_rows, LANES), bf16),
                pltpu.VMEM((tiles * 8, LANES), f32),
                pltpu.VMEM((2, 2 * local_count * turned_tiles * LANES, units), bf16),
                pltpu.VMEM((rows, out_cuts[0][1] * LANES), f32),
                pltpu.VMEM((local_count, 4, peers, LANES), f32),
                dma((len(in_cuts), local_count, 2)),
                dma((pieces,)),
                dma((3,)),
                dma((len(in_cuts),)),
                dma((len(in_cuts),)),
                dma(()),
                dma(()),
                dma((local_count, others)),
                dma((local_count, others)),
                dma((pieces,)),
                dma((pieces,)),
            ],
            compiler_params=pltpu.CompilerParams(
                collective_id=0, has_side_effects=True, vmem_limit_bytes=64000 * 1024
            ),
        )(tokens, expert_ids, gate_weights, gate_proj, up_proj, down_proj)

    placed = (
        P(("groups", "expert", "tensor"), "sub"),
        P(("groups", "expert", "tensor"), None),
        P(("groups", "expert", "tensor"), None),
        P("expert", "tensor", "sub"),
        P("expert", "tensor", "sub"),
        P("expert", "tensor", "sub"),
    )
    return jax.shard_map(
        per_device,
        mesh=mesh,
        in_specs=placed,
        out_specs=P(("groups", "expert", "tensor"), "sub"),
        check_vma=False,
    )
```
